32 devices in a mesh: ops: 8 (over z, x), sec: 4 (over y, core).
Axes of the slice: x: 2, y: 2, z: 4, core: 2. Of those that a mesh axis runs over, the one named last changes fastest.
Arguments:
- operators: bfloat16 [16, 8, 768, 768], P('ops', 'sec'), may hold values from -6 to 6
- basis: bfloat16 [8, 768, 768], P('sec'), may hold values from -0.21875 to 0.21875
- shift: int32 [16], replicated, may hold values from -1 to 1
- dest: int32 [16], replicated, may hold values from 0 to 15, each once
- sector_sizes: int32 [8], replicated, may hold values from 384 to 768
Outputs:
- renormalized: bfloat16 [16, 8, 768, 768], P('ops', 'sec')
The draws below stay inside these ranges and needn't reach their ends.
Inputs may be any that keep to these rules, and one draw needn't show every extreme that they name: `shift`: each pair's offset is -1, 0 or 1. dest names every index of 0 to 15 once.
All inputs are finite; a program needn't handle non-finite values.
Results may differ from the reference program's by a relative error of at most 0.0049.
Values may be sent and summed in bfloat16 or wider, within the bound.
A program may use at most 128 MiB of HBM per device.

```python
import jax
import jax.numpy as jnp
from jax import lax

M = 768
NSEC = 8
PAIRS = 16


def touch_ends(array, stream_key, smallest, largest):
    shape = array.shape
    index_at = [jax.random.randint(jax.random.fold_in(stream_key, axis), (), 0, shape[axis]) for axis in range(len(shape))]
    array = array.at[tuple(index_at)].set(smallest)
    longest = shape.index(max(shape))
    index_at[longest] = (index_at[longest] + 1) % shape[longest]
    return array.at[tuple(index_at)].set(largest)


def steps_of(own_key, dims, split, smallest, high):
    def one(dim, parts):
        draws = jax.random.uniform(jax.random.fold_in(jax.random.fold_in(own_key, 6), dim), (parts,), jnp.float32, smallest / len(split), high / len(split))
        return jnp.repeat(jnp.exp(draws), dims[dim] // parts).reshape((-1,) + (1,) * (len(dims) - dim - 1))

    level = one(*split[0])
    for cut in split[1:]:
        level = level * one(*cut)
    return level


def noise(own_key, dims, scale, limit, shards=(), held_as=jnp.bfloat16):
    result = jax.random.normal(own_key, dims, jnp.float32) * scale
    if len(shards) > 0:
        result = steps_of(own_key, dims, shards, -0.22, 0.18) * result
    return jnp.clip(result, min=-limit, max=limit).astype(held_as)


def setup_inputs(seed: int = 0) -> dict:
    splits = jax.random.split(jax.random.key(seed), 6)
    return {
        "operators": noise(splits[0], (PAIRS, NSEC, M, M), 1.0, 6.0, ((0, 8), (1, 4))),
        "basis": noise(splits[1], (NSEC, M, M), M ** -0.5, 0.21875, ((0, 4),)),
        "shift": touch_ends(jax.random.randint(splits[2], (PAIRS,), -1, 2), jax.random.fold_in(splits[2], 1), -1, 1).astype(jnp.int32),
        "dest": jax.random.permutation(splits[3], PAIRS).astype(jnp.int32),
        "sector_sizes": touch_ends(jax.random.randint(splits[4], (NSEC,), M // 2, M + 1), jax.random.fold_in(splits[4], 1), M // 2, M).astype(jnp.int32),
    }


def reference(operators, basis, shift, dest, sector_sizes):
    columns = jnp.arange(M, dtype=jnp.int32)
    kept = columns[None, :] < sector_sizes[:, None]
    kept_basis = jnp.where(kept[:, None, :], basis, jnp.zeros_like(basis))
    sector_ids = jnp.arange(NSEC, dtype=jnp.int32)

    def rotate_pair(packed):
        blocks, offset = packed
        target = (sector_ids + offset) % NSEC

        def one_sector(index):
            block = lax.dynamic_index_in_dim(blocks, index, 0, False)
            own = lax.dynamic_index_in_dim(kept_basis, index, 0, False)
            other = lax.dynamic_index_in_dim(kept_basis, target[index], 0, False)
            half = jnp.dot(block, own, preferred_element_type=jnp.float32).astype(jnp.bfloat16)
            return jnp.dot(other.T, half, preferred_element_type=jnp.float32).astype(jnp.bfloat16)

        return lax.map(one_sector, sector_ids)

    rotated = lax.map(rotate_pair, (operators, shift))
    source = jnp.zeros((PAIRS,), jnp.int32).at[dest].set(jnp.arange(PAIRS, dtype=jnp.int32))
    return jnp.take(rotated, source, axis=0)
```

```python
import functools

import jax
import jax.numpy as jnp
from jax import lax
from jax.experimental import pallas as pl
from jax.experimental.pallas import tpu as pltpu
from jax.sharding import PartitionSpec as P

MESH = pl.DeviceIdType.MESH
GRAIN = 16
TILES = 6
LAG = 2
SLOTS = 2 * LAG
STAGES = 2
SPARE = 16
ROUNDS = (20, 22, 24, 26, 28, 30, 32, 34, 36, 38, 40, 42, 44, 47, 50, 54, 60, 78)
RIGHT, LEFT, CROSS = 0, 1, 2


def plan_kernel(
    devices, per, sectors, full, limit, dest_ref, shift_ref, sizes_ref,
    table_ref, final_ref, length_ref, offset_ref,
    node, ready, via, order, cursor,
):
    me = lax.axis_index("ops")
    first = lax.axis_index("sec") * sectors
    own = per * sectors * full
    pairs = devices * per

    def clear(ref, size):
        def one(i, _):
            ref[i] = 0
            return 0

        lax.fori_loop(0, size, one, 0, unroll=8)

    clear(table_ref, table_ref.shape[0])
    clear(final_ref, own)
    clear(cursor, devices * 3)
    length_ref[0] = 0

    def units(sector):
        return lax.div(sizes_ref[sector] + (GRAIN - 1), GRAIN)

    total = sizes_ref.shape[0]
    length = units(0) + units(1)
    for s in range(sectors, total, sectors):
        length = jnp.maximum(length, units(s) + units(s + 1))
    head = units(first)
    held = head + units(first + 1)
    cut = lax.div(length, 2)
    jump = full - head

    def stay(pair, _):
        there = dest_ref[pair]
        offset_ref[there] = shift_ref[pair]

        @pl.when((lax.div(pair, per) == me) & (lax.div(there, per) == me))
        def _():
            source = lax.rem(pair, per) * (sectors * full)
            target = lax.rem(there, per) * (sectors * full)

            def one(i, _):
                final_ref[target + i] = source + i
                return 0

            lax.fori_loop(0, sectors * full, one, 0, unroll=8)

        return 0

    lax.fori_loop(0, pairs, stay, 0)

    def rank(step, at):
        far = devices // 2 - 1 - step

        def visit(pair, at):
            here, there = lax.div(pair, per), lax.div(dest_ref[pair], per)
            gap = lax.shift_right_logical(there, 1) - lax.shift_right_logical(here, 1)
            hit = (jnp.abs(gap) == far) & (here != there)

            @pl.when(hit)
            def _():
                split = gap != 0
                lead = pair * 2 + jnp.where(split, 0, here & 1)
                order[at] = lead
                order[at + 1] = pair * 2 + 1
                for i in (pair * 2, pair * 2 + 1):
                    node[i] = here
                    ready[i] = 0

            return at + jnp.where(hit, jnp.where(gap != 0, 2, 1), 0)

        return lax.fori_loop(0, pairs, visit, at)

    moving = lax.fori_loop(0, devices // 2, rank, jnp.int32(0))

    def one_hop(carry):
        hop, active = carry

        def visit(k, left):
            i = order[k]
            pair, column = lax.shift_right_logical(i, 1), i & 1
            goal = dest_ref[pair]
            there = lax.div(goal, per)
            begin = lax.div(pair, per)
            here = node[i]
            z, x = lax.shift_right_logical(here, 1), here & 1
            far = lax.shift_right_logical(there, 1)
            split = far != lax.shift_right_logical(begin, 1)
            offset = jnp.where(split & (column == 1), cut, 0)
            size = jnp.where(split, jnp.where(column == 1, length - cut, cut), length)
            along = (far != z) & (x == column)
            way = jnp.where(along, jnp.where(far > z, RIGHT, LEFT), CROSS)
            now = jnp.where(along, jnp.where(far > z, here + 2, here - 2), here ^ 1)
            lane = here * 3 + way
            free = ready[i]
            start = jnp.maximum(cursor[lane], free)
            stop = start + size
            cursor[lane] = stop
            length_ref[0] = jnp.maximum(length_ref[0], stop)
            mine = (here == me) & (stop <= limit)

            @pl.when(mine & (hop == 0))
            def _():
                base = lax.rem(pair, per) * (sectors * full)

                def four(c, _):
                    for u in range(4):
                        j = offset + c * 4 + u
                        table_ref[(start + c * 4 + u) * 3 + way] = (
                            base + j + jnp.where(j >= head, jump, 0)
                        )
                    return 0

                lax.fori_loop(0, lax.div(size + 3, 4), four, 0)

            @pl.when(mine & (hop > 0))
            def _():
                base = own + via[i] + 3 * (free - LAG * TILES)

                def four(c, _):
                    for u in range(4):
                        j = (c * 4 + u) * 3
                        table_ref[start * 3 + way + j] = base + j
                    return 0

                lax.fori_loop(0, lax.div(size + 3, 4), four, 0)

            @pl.when((now == there) & (now == me) & (stop <= limit))
            def _():
                base = lax.rem(goal, per) * (sectors * full)

                def one(u, _):
                    j = offset + u
                    final_ref[base + j + jnp.where(j >= head, jump, 0)] = (
                        own + way + 3 * (start + u)
                    )
                    return 0

                lax.fori_loop(0, jnp.clip(held - offset, 0, size), one, 0)

            node[i] = now
            via[i] = way
            ready[i] = start + LAG * TILES
            order[left] = i
            return left + (now != there).astype(jnp.int32)

        return hop + 1, lax.fori_loop(0, active, visit, jnp.int32(0))

    lax.while_loop(lambda carry: carry[1] > 0, one_hop, (jnp.int32(0), moving))


def plan(dest, shift, sizes, devices, per, sectors, full, limit):
    pairs = devices * per
    smem = pl.BlockSpec(memory_space=pltpu.SMEM)
    return pl.pallas_call(
        functools.partial(plan_kernel, devices, per, sectors, full, limit),
        out_shape=(
            jax.ShapeDtypeStruct((3 * (limit + SPARE),), jnp.int32),
            jax.ShapeDtypeStruct((per * sectors * full,), jnp.int32),
            jax.ShapeDtypeStruct((1,), jnp.int32),
            jax.ShapeDtypeStruct((pairs,), jnp.int32),
        ),
        in_specs=[smem] * 3,
        out_specs=(smem,) * 4,
        scratch_shapes=[pltpu.SMEM((2 * pairs,), jnp.int32)] * 3
        + [pltpu.SMEM((2 * pairs + 1,), jnp.int32), pltpu.SMEM((devices * 3,), jnp.int32)],
    )(dest, shift, sizes)


def route_kernel(
    rounds, devices, table_ref, final_ref, blocks_ref, out_ref,
    pool, stage, recv, own_sem, send_sem, recv_sem,
):
    own = blocks_ref.shape[0]
    me = lax.axis_index("ops")
    z, x = me // 2, me % 2
    has = (z < devices // 2 - 1, z > 0, x >= 0)
    back = (has[LEFT], has[RIGHT], has[CROSS])
    to = (me + 2, me - 2, me + 1 - 2 * x)
    peers = 1 + has[RIGHT].astype(jnp.int32) + has[LEFT].astype(jnp.int32)

    load = pltpu.make_async_copy(blocks_ref, pool.at[pl.ds(0, own)], own_sem)
    load.start()
    barrier = pltpu.get_barrier_semaphore()
    for d in range(3):

        @pl.when(has[d])
        def _():
            pl.semaphore_signal(barrier, inc=1, device_id={"ops": to[d]}, device_id_type=MESH)

    load.wait()
    pl.semaphore_wait(barrier, peers)

    def copy(r, d):
        here, there = lax.rem(r, STAGES), lax.rem(r, SLOTS)
        return pltpu.make_async_remote_copy(
            src_ref=stage.at[here, d],
            dst_ref=recv.at[there, d],
            send_sem=send_sem.at[here, d],
            recv_sem=recv_sem.at[there, d],
            device_id={"ops": to[d]},
            device_id_type=MESH,
        )

    def sent(r):
        for d in range(3):

            @pl.when(has[d])
            def _():
                copy(r, d).wait_send()

    def send(r):
        here = lax.rem(r, STAGES)
        for d in range(3):
            for t in range(TILES):
                stage[here, d, t] = pool[table_ref[(r * TILES + t) * 3 + d]]
        for d in range(3):

            @pl.when(has[d])
            def _():
                copy(r, d).start()

    def collect(r):
        there = lax.rem(r, SLOTS)
        for d in range(3):

            @pl.when(back[d])
            def _():
                copy(r, d).wait_recv()
                for t in range(TILES):
                    pool[own + (r * TILES + t) * 3 + d] = recv[there, d, t]

    for r in range(LAG - 1):
        send(jnp.int32(r))

    def step(r, _):
        @pl.when(r >= STAGES)
        def _():
            sent(r - STAGES)

        send(r)
        collect(r - (LAG - 1))
        return 0

    lax.fori_loop(LAG - 1, rounds, step, 0)
    for r in range(rounds - LAG + 1, rounds):
        collect(jnp.int32(r))
    for r in range(rounds - STAGES, rounds):
        sent(jnp.int32(r))

    def finish(i, _):
        for u in range(4):
            out_ref[i * 4 + u] = pool[final_ref[i * 4 + u]]
        return 0

    lax.fori_loop(0, own // 4, finish, 0)


def route(rounds, devices, table, final, blocks):
    width, columns = blocks.shape[2:]
    own = blocks.size // (GRAIN * columns)
    dtype = blocks.dtype
    smem = pl.BlockSpec(memory_space=pltpu.SMEM)
    out = pl.pallas_call(
        functools.partial(route_kernel, rounds, devices),
        out_shape=jax.ShapeDtypeStruct((own, GRAIN, columns), dtype),
        in_specs=[smem, smem, pl.BlockSpec(memory_space=pl.ANY)],
        out_specs=pl.BlockSpec(memory_space=pltpu.VMEM),
        scratch_shapes=[
            pltpu.VMEM((own + 3 * rounds * TILES + SPARE, GRAIN, columns), dtype),
            pltpu.VMEM((STAGES, 3, TILES, GRAIN, columns), dtype),
            pltpu.VMEM((SLOTS, 3, TILES, GRAIN, columns), dtype),
            pltpu.SemaphoreType.DMA,
            pltpu.SemaphoreType.DMA((STAGES, 3)),
            pltpu.SemaphoreType.DMA((SLOTS, 3)),
        ],
        compiler_params=pltpu.CompilerParams(
            collective_id=rounds, has_side_effects=True, vmem_limit_bytes=60 * 1024 * 1024
        ),
    )(table, final, blocks.reshape(own, GRAIN, columns))
    return out.reshape(blocks.shape)


def exchange(blocks, dest):
    pair_dev, sector_dev, width = blocks.shape[:3]
    ops_count = lax.axis_size("ops")
    strip = width // ops_count
    source = jnp.argsort(dest, stable=True)
    split = blocks.reshape(pair_dev, sector_dev, ops_count, strip, blocks.shape[3])
    spread = lax.all_to_all(split, "ops", split_axis=2, concat_axis=0, tiled=True)
    ordered = jnp.take(spread, source, axis=0)
    returned = lax.all_to_all(ordered, "ops", split_axis=0, concat_axis=2, tiled=True)
    return returned.reshape(blocks.shape)


def reassign(blocks, dest, shift, sector_sizes):
    devices = lax.axis_size("ops")
    per, sectors, width, _ = blocks.shape
    if devices > 12 or devices % 2 or width % GRAIN or sectors != 2:
        offsets = jnp.take(shift, jnp.argsort(dest, stable=True))
        return exchange(blocks, dest), offsets
    limit = max(ROUNDS) * TILES
    full = width // GRAIN
    table, final, length, offsets = plan(
        dest, shift, sector_sizes, devices, per, sectors, full, limit
    )
    index = sum((length[0] > r * TILES).astype(jnp.int32) for r in ROUNDS)
    branches = [functools.partial(route, r, devices) for r in ROUNDS]
    branches.append(lambda table, final, blocks: exchange(blocks, dest))
    return lax.switch(index, branches, table, final, blocks), offsets


def half_kernel(basis_ref, block_ref, out_ref):
    half = lax.dot_general(
        basis_ref[0], block_ref[0, 0], (((0,), (1,)), ((), ())),
        preferred_element_type=jnp.float32,
    )
    out_ref[0, 0] = half.astype(out_ref.dtype)


def halve(operators, basis):
    per, sectors, width, columns = operators.shape
    one = pl.BlockSpec((1, 1, width, columns), lambda s, p: (p, s, 0, 0))
    return pl.pallas_call(
        half_kernel,
        grid=(sectors, per),
        out_shape=jax.ShapeDtypeStruct(operators.shape, operators.dtype),
        in_specs=[pl.BlockSpec((1, width, columns), lambda s, p: (s, 0, 0)), one],
        out_specs=one,
        cost_estimate=pl.CostEstimate(
            flops=2 * per * sectors * width**3, bytes_accessed=5 * operators.size,
            transcendentals=0,
        ),
    )(basis, operators)


def rotate_kernel(
    total, offset_ref, sizes_ref, low_ref, basis_ref, high_ref, block_ref, out_ref, near, sem
):
    per, sectors = pl.num_programs(0), pl.num_programs(1)
    p, s = pl.program_id(0), pl.program_id(1)
    count = basis_ref.shape[0]

    @pl.when((p == 0) & (s == 0))
    def _():
        copies = [
            pltpu.make_async_copy(low_ref, near.at[pl.ds(0, 1)], sem.at[0]),
            pltpu.make_async_copy(basis_ref, near.at[pl.ds(1, count)], sem.at[1]),
            pltpu.make_async_copy(high_ref, near.at[pl.ds(count + 1, 1)], sem.at[2]),
        ]
        for copy in copies:
            copy.start()
        for copy in copies:
            copy.wait()

    offset = offset_ref[lax.axis_index("ops") * per + p]
    sector = lax.axis_index("sec") * sectors + s
    kept_columns = sizes_ref[sector]
    kept_rows = sizes_ref[lax.rem(sector + offset + total, total)]
    full = lax.dot_general(
        near[1 + s + offset], block_ref[0, 0], (((0,), (1,)), ((), ())),
        preferred_element_type=jnp.float32,
    )
    row = lax.broadcasted_iota(jnp.int32, full.shape, 0)
    column = lax.broadcasted_iota(jnp.int32, full.shape, 1)
    full = jnp.where((row < kept_rows) & (column < kept_columns), full, 0.0)
    out_ref[0, 0] = full.astype(out_ref.dtype)


def rotate(blocks, low, basis, high, offsets, sector_sizes, total):
    per, sectors, width, columns = blocks.shape
    smem = pl.BlockSpec(memory_space=pltpu.SMEM)
    hbm = pl.BlockSpec(memory_space=pl.ANY)
    one = pl.BlockSpec((1, 1, width, columns), lambda p, s: (p, s, 0, 0))
    return pl.pallas_call(
        functools.partial(rotate_kernel, total),
        grid=(per, sectors),
        out_shape=jax.ShapeDtypeStruct(blocks.shape, blocks.dtype),
        in_specs=[smem, smem, hbm, hbm, hbm, one],
        out_specs=one,
        scratch_shapes=[
            pltpu.VMEM((sectors + 2, width, columns), blocks.dtype),
            pltpu.SemaphoreType.DMA((3,)),
        ],
        cost_estimate=pl.CostEstimate(
            flops=2 * per * sectors * width**3, bytes_accessed=4 * blocks.size, transcendentals=0
        ),
    )(offsets, sector_sizes, low, basis, high, blocks)


def body(operators, basis, shift, dest, sector_sizes):
    count = lax.axis_size("sec")
    forward = [(i, (i + 1) % count) for i in range(count)]
    backward = [(target, source) for source, target in forward]
    low = lax.ppermute(basis[-1:], "sec", forward)
    high = lax.ppermute(basis[:1], "sec", backward)
    halves = halve(operators, basis)
    blocks, offsets = reassign(halves, dest, shift, sector_sizes)
    total = basis.shape[0] * count
    return rotate(blocks, low, basis, high, offsets, sector_sizes, total)


def solution(mesh):
    return jax.shard_map(
        body,
        mesh=mesh,
        in_specs=(P("ops", "sec", None, None), P("sec", None, None), P(), P(), P()),
        out_specs=P("ops", "sec", None, None),
        check_vma=False,
    )
```

```python
import functools

import jax
import jax.numpy as jnp
from jax import lax
from jax.experimental import pallas as pl
from jax.experimental.pallas import tpu as pltpu
from jax.sharding import PartitionSpec as P

MESH = pl.DeviceIdType.MESH
GRAIN = 16
TILES = 5
LAG = 2
SLOTS = 2 * LAG
STAGES = 2
BIAS = 8
BITS = 11
ROUNDS = (20, 22, 24, 26, *range(28, 52), 54, 57, 61, 67, 76, 93)
RIGHT, LEFT, CROSS = 0, 1, 2


def over(value, unit):
    if unit & (unit - 1) == 0:
        return lax.shift_right_logical(value, unit.bit_length() - 1)
    return lax.shift_right_logical(value * (65536 // unit + 1), 16)


def plan(
    devices, per, sectors, full, limit, dest_ref, shift_ref, sizes_ref,
    table_ref, final_ref, index_ref, offset_ref,
    node, ready, source, order, cursor,
):
    me = lax.axis_index("ops")
    held = sectors * full
    own = per * held
    pairs = devices * per
    chunks = limit // TILES

    def empty(i, _):
        table_ref[i] = BIAS + (BIAS << BITS)
        return 0

    lax.fori_loop(0, 3 * chunks, empty, 0, unroll=6)
    for i in range(devices * 3):
        cursor[i] = 0

    def units(sector):
        return over(sizes_ref[sector] + (GRAIN - 1), GRAIN)

    total = sizes_ref.shape[0]
    length = units(0) + units(1)
    for s in range(sectors, total, sectors):
        length = jnp.maximum(length, units(s) + units(s + 1))
    cut = over(length, 2)

    def stay(pair, _):
        there = dest_ref[pair]
        offset_ref[there] = shift_ref[pair]

        @pl.when((over(pair, per) == me) & (over(there, per) == me))
        def _():
            slot = (there - over(there, per) * per) * 3
            final_ref[slot] = (pair - over(pair, per) * per) * held
            final_ref[slot + 1] = 0
            final_ref[slot + 2] = held

        return 0

    lax.fori_loop(0, pairs, stay, 0)

    def rank(step, at):
        far = devices // 2 - 1 - step

        def visit(pair, at):
            here, there = over(pair, per), over(dest_ref[pair], per)
            gap = lax.shift_right_logical(there, 1) - lax.shift_right_logical(here, 1)
            hit = (jnp.abs(gap) == far) & (here != there)
            split = gap != 0

            @pl.when(hit)
            def _():
                order[at] = pair * 2 + jnp.where(split, 0, here & 1)
                order[at + 1] = pair * 2 + 1
                for c in range(2):
                    i = pair * 2 + c
                    node[i] = here
                    ready[i] = 0
                    source[i] = (pair - over(pair, per) * per) * held + jnp.where(split & (c == 1), cut, 0)

            return at + jnp.where(hit, jnp.where(split, 2, 1), 0)

        return lax.fori_loop(0, pairs, visit, at)

    moving = lax.fori_loop(0, devices // 2, rank, jnp.int32(0))

    def one_hop(carry):
        active, longest = carry

        def visit(k, carry):
            left, longest = carry
            i = order[k]
            pair, column = lax.shift_right_logical(i, 1), i & 1
            goal = dest_ref[pair]
            there = over(goal, per)
            here = node[i]
            z, x = lax.shift_right_logical(here, 1), here & 1
            far = lax.shift_right_logical(there, 1)
            split = far != lax.shift_right_logical(over(pair, per), 1)
            size = jnp.where(split, jnp.where(column == 1, length - cut, cut), length)
            along = (far != z) & (x == column)
            way = jnp.where(along, jnp.where(far > z, RIGHT, LEFT), CROSS)
            now = jnp.where(along, jnp.where(far > z, here + 2, here - 2), here ^ 1)
            lane = here * 3 + way
            start = jnp.maximum(cursor[lane], ready[i])
            stop = start + size
            cursor[lane] = stop
            begin = source[i]
            arrived = own + way * limit + start

            @pl.when((here == me) & (stop <= limit))
            def _():
                chunk = over(start, TILES)
                base = begin - start + chunk * TILES + BIAS
                at = chunk * 3 + way
                keep = table_ref[at] & ((1 << BITS) - 1)
                table_ref[at] = keep + (base << BITS) + ((start - chunk * TILES) << (2 * BITS))
                last = over(stop - 1, TILES)

                def one(c, _):
                    word = base + (c - chunk) * TILES + (TILES << (2 * BITS))
                    table_ref[c * 3 + way] = word
                    return 0

                lax.fori_loop(chunk + 1, last + 1, one, 0)

            @pl.when((now == there) & (now == me) & (stop <= limit))
            def _():
                slot = (goal - there * per) * 3
                final_ref[slot + 2] = jnp.where(split, cut, held)

                @pl.when(split & (column == 1))
                def _():
                    final_ref[slot + 1] = arrived - cut

                @pl.when(jnp.logical_not(split & (column == 1)))
                def _():
                    final_ref[slot] = arrived

                @pl.when(jnp.logical_not(split))
                def _():
                    final_ref[slot + 1] = 0

            node[i] = now
            source[i] = arrived
            ready[i] = start + LAG * TILES
            order[left] = i
            return left + (now != there).astype(jnp.int32), jnp.maximum(longest, stop)

        return lax.fori_loop(0, active, visit, (jnp.int32(0), longest))

    _, longest = lax.while_loop(
        lambda carry: carry[0] > 0, one_hop, (moving, jnp.int32(0))
    )

    @pl.when(longest > limit)
    def _():
        for i in range(3 * per):
            final_ref[i] = 0

    index = jnp.int32(0)
    for r in ROUNDS:
        index = index + (longest > r * TILES).astype(jnp.int32)
    index_ref[0] = index


def prepare_kernel(
    devices, full, limit, dest_ref, shift_ref, sizes_ref, basis_ref, block_ref,
    table_ref, final_ref, index_ref, offset_ref, out_ref, *scratch,
):
    count = out_ref.shape[1] // (full * GRAIN)

    @pl.when((pl.program_id(0) == 0) & (pl.program_id(1) == 0))
    def _():
        plan(
            devices, dest_ref.shape[0] // devices, count, full, limit,
            dest_ref, shift_ref, sizes_ref, table_ref, final_ref, index_ref, offset_ref, *scratch,
        )

    half_kernel(sizes_ref, basis_ref, block_ref, out_ref)


def prepare(operators, basis, dest, shift, sizes, devices, limit):
    per, sectors, width, columns = operators.shape
    pairs = devices * per
    smem = pl.BlockSpec(memory_space=pltpu.SMEM)
    return pl.pallas_call(
        functools.partial(prepare_kernel, devices, width // GRAIN, limit),
        grid=(per, sectors),
        out_shape=(
            jax.ShapeDtypeStruct((3 * limit // TILES,), jnp.int32),
            jax.ShapeDtypeStruct((3 * per,), jnp.int32),
            jax.ShapeDtypeStruct((1,), jnp.int32),
            jax.ShapeDtypeStruct((pairs,), jnp.int32),
            jax.ShapeDtypeStruct((per, sectors * width, columns), operators.dtype),
        ),
        in_specs=[smem] * 3
        + [
            pl.BlockSpec(basis.shape, lambda p, s: (0, 0, 0)),
            pl.BlockSpec((1, 1, width, columns), lambda p, s: (p, s, 0, 0)),
        ],
        out_specs=(smem,) * 4
        + (pl.BlockSpec((1, sectors * width, columns), lambda p, s: (p, 0, 0)),),
        scratch_shapes=[pltpu.SMEM((2 * pairs,), jnp.int32)] * 3
        + [pltpu.SMEM((2 * pairs + 1,), jnp.int32), pltpu.SMEM((devices * 3,), jnp.int32)],
    )(dest, shift, sizes, basis, operators)


def route_kernel(
    rounds, devices, limit, table_ref, final_ref, blocks_ref, basis_ref, out_ref, edge_ref,
    pool, stage, recv, own_sem, send_sem, recv_sem, edge_send, edge_recv,
):
    own = blocks_ref.shape[0]
    per = final_ref.shape[0] // 3
    held = own // per
    me = lax.axis_index("ops")
    z, x = me // 2, me % 2
    has = (z < devices // 2 - 1, z > 0, x >= 0)
    back = (has[LEFT], has[RIGHT], has[CROSS])
    to = (me + 2, me - 2, me + 1 - 2 * x)
    count = lax.axis_size("sec")
    sec = lax.axis_index("sec")
    beside = (lax.rem(sec + 1, count), lax.rem(sec + count - 1, count))
    peers = 3 + has[RIGHT].astype(jnp.int32) + has[LEFT].astype(jnp.int32)

    load = pltpu.make_async_copy(blocks_ref, pool.at[pl.ds(0, own)], own_sem)
    load.start()
    barrier = pltpu.get_barrier_semaphore()
    for d in range(3):

        @pl.when(has[d])
        def _():
            pl.semaphore_signal(barrier, inc=1, device_id={"ops": to[d]}, device_id_type=MESH)

    for b in beside:
        pl.semaphore_signal(barrier, inc=1, device_id={"sec": b}, device_id_type=MESH)
    pl.semaphore_wait(barrier, peers)
    edges = [
        pltpu.make_async_remote_copy(
            src_ref=basis_ref.at[basis_ref.shape[0] - 1 if side == 0 else 0],
            dst_ref=edge_ref.at[side],
            send_sem=edge_send.at[side],
            recv_sem=edge_recv.at[side],
            device_id={"sec": beside[side]},
            device_id_type=MESH,
        )
        for side in range(2)
    ]
    for edge in edges:
        edge.start()
    load.wait()

    def copy(r, d):
        here, there = lax.rem(r, STAGES), lax.rem(r, SLOTS)
        return pltpu.make_async_remote_copy(
            src_ref=stage.at[here, d],
            dst_ref=recv.at[there, d],
            send_sem=send_sem.at[here, d],
            recv_sem=recv_sem.at[there, d],
            device_id={"ops": to[d]},
            device_id_type=MESH,
        )

    def sent(r):
        for d in range(3):

            @pl.when(has[d])
            def _():
                copy(r, d).wait_send()

    def send(r):
        here = lax.rem(r, STAGES)
        for d in range(3):
            word = table_ref[r * 3 + d]
            one = (word & ((1 << BITS) - 1)) - BIAS
            two = (lax.shift_right_logical(word, BITS) & ((1 << BITS) - 1)) - BIAS
            turn = lax.shift_right_logical(word, 2 * BITS)
            for t in range(TILES):
                stage[here, d, t] = pool[jnp.maximum(jnp.where(t < turn, one, two) + t, 0)]
        for d in range(3):

            @pl.when(has[d])
            def _():
                copy(r, d).start()

    def collect(r):
        there = lax.rem(r, SLOTS)
        for d in range(3):

            @pl.when(back[d])
            def _():
                copy(r, d).wait_recv()
                for t in range(TILES):
                    pool[own + d * limit + r * TILES + t] = recv[there, d, t]

    for r in range(LAG - 1):
        send(jnp.int32(r))

    def step(r, _):
        @pl.when(r >= STAGES)
        def _():
            sent(r - STAGES)

        send(r)
        collect(r - (LAG - 1))
        return 0

    lax.fori_loop(LAG - 1, rounds, step, 0)
    for r in range(rounds - LAG + 1, rounds):
        collect(jnp.int32(r))

    for q in range(per):
        one, two, turn = final_ref[q * 3], final_ref[q * 3 + 1], final_ref[q * 3 + 2]

        def finish(i, _):
            for u in range(4):
                k = i * 4 + u
                at = jnp.where(k < turn, one, two) + k
                out_ref[q * held + k] = pool[jnp.clip(at, 0, own + 3 * limit)]
            return 0

        lax.fori_loop(0, held // 4, finish, 0)
    for r in range(rounds - STAGES, rounds):
        sent(jnp.int32(r))
    for edge in edges:
        edge.wait()


def route(rounds, devices, limit, table, final, lists, basis):
    own, _, columns = lists.shape
    dtype = lists.dtype
    smem = pl.BlockSpec(memory_space=pltpu.SMEM)
    hbm = pl.BlockSpec(memory_space=pl.ANY)
    return pl.pallas_call(
        functools.partial(route_kernel, rounds, devices, limit),
        out_shape=(
            jax.ShapeDtypeStruct(lists.shape, dtype),
            jax.ShapeDtypeStruct((2, *basis.shape[1:]), dtype),
        ),
        in_specs=[smem, smem, hbm, hbm],
        out_specs=(pl.BlockSpec(memory_space=pltpu.VMEM), hbm),
        scratch_shapes=[
            pltpu.VMEM((own + 3 * limit + 1, GRAIN, columns), dtype),
            pltpu.VMEM((STAGES, 3, TILES, GRAIN, columns), dtype),
            pltpu.VMEM((SLOTS, 3, TILES, GRAIN, columns), dtype),
            pltpu.SemaphoreType.DMA,
            pltpu.SemaphoreType.DMA((STAGES, 3)),
            pltpu.SemaphoreType.DMA((SLOTS, 3)),
            pltpu.SemaphoreType.DMA((2,)),
            pltpu.SemaphoreType.DMA((2,)),
        ],
        compiler_params=pltpu.CompilerParams(
            collective_id=rounds, has_side_effects=True, vmem_limit_bytes=60 * 1024 * 1024
        ),
    )(table, final, lists, basis)


def edges_of(basis):
    count = lax.axis_size("sec")
    forward = [(i, (i + 1) % count) for i in range(count)]
    backward = [(target, source) for source, target in forward]
    low = lax.ppermute(basis[-1:], "sec", forward)
    high = lax.ppermute(basis[:1], "sec", backward)
    return jnp.concatenate([low, high])


def exchange(lists, dest, per):
    ops_count = lax.axis_size("ops")
    source = jnp.argsort(dest, stable=True)
    blocks = lists.reshape(per, ops_count, -1, lists.shape[2])
    spread = lax.all_to_all(blocks, "ops", split_axis=1, concat_axis=0, tiled=True)
    ordered = jnp.take(spread, source, axis=0)
    returned = lax.all_to_all(ordered, "ops", split_axis=0, concat_axis=1, tiled=True)
    return returned.reshape(lists.shape)


def reassign(operators, basis, dest, shift, sizes):
    devices = lax.axis_size("ops")
    per, sectors, width, columns = operators.shape
    own = per * sectors * (width // GRAIN)

    def plain(lists, basis):
        return exchange(lists, dest, per), edges_of(basis)

    if devices > 12 or devices % 2 or sectors != 2:
        lists = halve(operators, basis, sizes).reshape(own, GRAIN, columns)
        offsets = jnp.take(shift, jnp.argsort(dest, stable=True))
        return *plain(lists, basis), offsets
    limit = max(ROUNDS) * TILES
    table, final, index, offsets, lists = prepare(
        operators, basis, dest, shift, sizes, devices, limit
    )
    lists = lists.reshape(own, GRAIN, columns)
    branches = [functools.partial(route, r, devices, limit) for r in ROUNDS]
    branches.append(lambda table, final, lists, basis: plain(lists, basis))
    out, edge = lax.switch(index[0], branches, table, final, lists, basis)
    return out, edge, offsets


def half_kernel(sizes_ref, basis_ref, block_ref, out_ref):
    sectors, width = basis_ref.shape[:2]
    s = pl.program_id(1)
    half = lax.dot_general(
        basis_ref[s], block_ref[0, 0], (((0,), (1,)), ((), ())),
        preferred_element_type=jnp.float32,
    )
    at = start_of(sizes_ref, sectors, s, width)
    out_ref[0, pl.ds(at, width), :] = half.astype(out_ref.dtype)


def start_of(sizes_ref, sectors, s, width):
    at = jnp.int32(0)
    for before in range(sectors - 1):
        size = sizes_ref[lax.axis_index("sec") * sectors + before]
        rows = lax.div(size + (GRAIN - 1), GRAIN) * GRAIN
        at = at + jnp.where(before < s, rows, 0)
    return pl.multiple_of(at, GRAIN)


def halve(operators, basis, sizes):
    per, sectors, width, columns = operators.shape
    smem = pl.BlockSpec(memory_space=pltpu.SMEM)
    return pl.pallas_call(
        half_kernel,
        grid=(per, sectors),
        out_shape=jax.ShapeDtypeStruct((per, sectors * width, columns), operators.dtype),
        in_specs=[
            smem,
            pl.BlockSpec(basis.shape, lambda p, s: (0, 0, 0)),
            pl.BlockSpec((1, 1, width, columns), lambda p, s: (p, s, 0, 0)),
        ],
        out_specs=pl.BlockSpec((1, sectors * width, columns), lambda p, s: (p, 0, 0)),
        cost_estimate=pl.CostEstimate(
            flops=2 * per * sectors * width**3, bytes_accessed=6 * operators.size,
            transcendentals=0,
        ),
    )(sizes, basis, operators)


def rotate_kernel(
    total, offset_ref, sizes_ref, edge_ref, basis_ref, list_ref, out_ref, near, sem
):
    per, sectors = pl.num_programs(0), pl.num_programs(1)
    p, s = pl.program_id(0), pl.program_id(1)
    count, width = basis_ref.shape[:2]

    @pl.when((p == 0) & (s == 0))
    def _():
        copies = [
            pltpu.make_async_copy(edge_ref.at[0], near.at[0], sem.at[0]),
            pltpu.make_async_copy(basis_ref, near.at[pl.ds(1, count)], sem.at[1]),
            pltpu.make_async_copy(edge_ref.at[1], near.at[count + 1], sem.at[2]),
        ]
        for copy in copies:
            copy.start()
        for copy in copies:
            copy.wait()

    offset = offset_ref[lax.axis_index("ops") * per + p]
    sector = lax.axis_index("sec") * sectors + s
    kept_columns = sizes_ref[sector]
    kept_rows = sizes_ref[lax.rem(sector + offset + total, total)]
    at = start_of(sizes_ref, count, s, width)
    full = lax.dot_general(
        near[1 + s + offset], list_ref[0, pl.ds(at, width), :], (((0,), (1,)), ((), ())),
        preferred_element_type=jnp.float32,
    )
    row = lax.broadcasted_iota(jnp.int32, full.shape, 0)
    column = lax.broadcasted_iota(jnp.int32, full.shape, 1)
    full = jnp.where((row < kept_rows) & (column < kept_columns), full, 0.0)
    out_ref[0, 0] = full.astype(out_ref.dtype)


def rotate(lists, basis, edge, offsets, sizes, shape, total):
    per, sectors, width, columns = shape
    smem = pl.BlockSpec(memory_space=pltpu.SMEM)
    hbm = pl.BlockSpec(memory_space=pl.ANY)
    return pl.pallas_call(
        functools.partial(rotate_kernel, total),
        grid=(per, sectors),
        out_shape=jax.ShapeDtypeStruct(shape, lists.dtype),
        in_specs=[
            smem, smem, hbm, hbm,
            pl.BlockSpec((1, sectors * width, columns), lambda p, s: (p, 0, 0)),
        ],
        out_specs=pl.BlockSpec((1, 1, width, columns), lambda p, s: (p, s, 0, 0)),
        scratch_shapes=[
            pltpu.VMEM((sectors + 2, width, columns), lists.dtype),
            pltpu.SemaphoreType.DMA((3,)),
        ],
        cost_estimate=pl.CostEstimate(
            flops=2 * per * sectors * width**3, bytes_accessed=5 * lists.size, transcendentals=0
        ),
    )(offsets, sizes, edge, basis, lists)


def body(operators, basis, shift, dest, sizes):
    per, sectors, width, columns = operators.shape
    total = sectors * lax.axis_size("sec")
    lists, edge, offsets = reassign(operators, basis, dest, shift, sizes)
    lists = lists.reshape(per, sectors * width, columns)
    return rotate(lists, basis, edge, offsets, sizes, operators.shape, total)


def solution(mesh):
    return jax.shard_map(
        body,
        mesh=mesh,
        in_specs=(P("ops", "sec", None, None), P("sec", None, None), P(), P(), P()),
        out_specs=P("ops", "sec", None, None),
        check_vma=False,
    )
```

```python
import functools

import jax
import jax.numpy as jnp
from jax import lax
from jax.experimental import pallas as pl
from jax.experimental.pallas import tpu as pltpu
from jax.sharding import PartitionSpec as P

MESH = pl.DeviceIdType.MESH
GRAIN = 16
TILES = 5
LAG = 2
SLOTS = 2 * LAG
STAGES = 2
BIAS = 8
BITS = 11
ROUNDS = (22, 26, 29, 31, 33, 35, *range(37, 44), 45, 47, 49, 52, 55, 60, 70, 93)
RIGHT, LEFT, CROSS = 0, 1, 2


def over(value, unit):
    if unit & (unit - 1) == 0:
        return lax.shift_right_logical(value, unit.bit_length() - 1)
    return lax.shift_right_logical(value * (65536 // unit + 1), 16)


def plan(
    devices, per, sectors, full, limit, dest_ref, shift_ref, sizes_ref,
    table_ref, final_ref, index_ref, offset_ref,
    node, ready, source, order, cursor,
):
    me = lax.axis_index("ops")
    held = sectors * full
    own = per * held
    pairs = devices * per
    chunks = limit // TILES

    def empty(i, _):
        table_ref[i] = BIAS + (BIAS << BITS)
        return 0

    lax.fori_loop(0, 3 * chunks, empty, 0, unroll=6)
    for i in range(devices * 3):
        cursor[i] = 0

    def units(sector):
        return over(sizes_ref[sector] + (GRAIN - 1), GRAIN)

    total = sizes_ref.shape[0]
    length = units(0) + units(1)
    for s in range(sectors, total, sectors):
        length = jnp.maximum(length, units(s) + units(s + 1))
    cut = over(length, 2)

    def stay(pair, _):
        there = dest_ref[pair]
        offset_ref[there] = shift_ref[pair]

        @pl.when((over(pair, per) == me) & (over(there, per) == me))
        def _():
            slot = (there - over(there, per) * per) * 3
            final_ref[slot] = (pair - over(pair, per) * per) * held
            final_ref[slot + 1] = 0
            final_ref[slot + 2] = held

        return 0

    lax.fori_loop(0, pairs, stay, 0)

    def rank(step, at):
        far = devices // 2 - 1 - step

        def visit(pair, at):
            here, there = over(pair, per), over(dest_ref[pair], per)
            gap = lax.shift_right_logical(there, 1) - lax.shift_right_logical(here, 1)
            hit = (jnp.abs(gap) == far) & (here != there)
            split = gap != 0

            @pl.when(hit)
            def _():
                order[at] = pair * 2 + jnp.where(split, 0, here & 1)
                order[at + 1] = pair * 2 + 1
                for c in range(2):
                    i = pair * 2 + c
                    node[i] = here
                    ready[i] = 0
                    source[i] = (pair - over(pair, per) * per) * held + jnp.where(split & (c == 1), cut, 0)

            return at + jnp.where(hit, jnp.where(split, 2, 1), 0)

        return lax.fori_loop(0, pairs, visit, at)

    moving = lax.fori_loop(0, devices // 2, rank, jnp.int32(0))

    def one_hop(carry):
        active, longest = carry

        def visit(k, carry):
            left, longest = carry
            i = order[k]
            pair, column = lax.shift_right_logical(i, 1), i & 1
            goal = dest_ref[pair]
            there = over(goal, per)
            here = node[i]
            z, x = lax.shift_right_logical(here, 1), here & 1
            far = lax.shift_right_logical(there, 1)
            split = far != lax.shift_right_logical(over(pair, per), 1)
            size = jnp.where(split, jnp.where(column == 1, length - cut, cut), length)
            along = (far != z) & (x == column)
            way = jnp.where(along, jnp.where(far > z, RIGHT, LEFT), CROSS)
            now = jnp.where(along, jnp.where(far > z, here + 2, here - 2), here ^ 1)
            lane = here * 3 + way
            start = jnp.maximum(cursor[lane], ready[i])
            stop = start + size
            cursor[lane] = stop
            begin = source[i]
            arrived = own + way * limit + start

            @pl.when((here == me) & (stop <= limit))
            def _():
                chunk = over(start, TILES)
                base = begin - start + chunk * TILES + BIAS
                at = chunk * 3 + way
                keep = table_ref[at] & ((1 << BITS) - 1)
                table_ref[at] = keep + (base << BITS) + ((start - chunk * TILES) << (2 * BITS))
                last = over(stop - 1, TILES)

                def one(c, _):
                    word = base + (c - chunk) * TILES + (TILES << (2 * BITS))
                    table_ref[c * 3 + way] = word
                    return 0

                lax.fori_loop(chunk + 1, last + 1, one, 0)

            @pl.when((now == there) & (now == me) & (stop <= limit))
            def _():
                slot = (goal - there * per) * 3
                final_ref[slot + 2] = jnp.where(split, cut, held)

                @pl.when(split & (column == 1))
                def _():
                    final_ref[slot + 1] = arrived - cut

                @pl.when(jnp.logical_not(split & (column == 1)))
                def _():
                    final_ref[slot] = arrived

                @pl.when(jnp.logical_not(split))
                def _():
                    final_ref[slot + 1] = 0

            node[i] = now
            source[i] = arrived
            ready[i] = start + LAG * TILES
            order[left] = i
            return left + (now != there).astype(jnp.int32), jnp.maximum(longest, stop)

        return lax.fori_loop(0, active, visit, (jnp.int32(0), longest))

    _, longest = lax.while_loop(
        lambda carry: carry[0] > 0, one_hop, (moving, jnp.int32(0))
    )

    @pl.when(longest > limit)
    def _():
        for i in range(3 * per):
            final_ref[i] = 0

    index = jnp.int32(0)
    for r in ROUNDS:
        index = index + (longest > r * TILES).astype(jnp.int32)
    index_ref[0] = index


def prepare_kernel(
    devices, full, limit, dest_ref, shift_ref, sizes_ref, basis_ref, block_ref,
    table_ref, final_ref, index_ref, offset_ref, out_ref, *scratch,
):
    count = basis_ref.shape[0]
    *scratch, basis, blocks, basis_sem, block_sem = scratch
    p, s = pl.program_id(0), pl.program_id(1)
    total = block_ref.shape[0]

    def load(b):
        return pltpu.make_async_copy(block_ref.at[b], blocks.at[b], block_sem.at[b])

    @pl.when((p == 0) & (s == 0))
    def _():
        own = pltpu.make_async_copy(basis_ref, basis, basis_sem)
        own.start()
        for b in range(total):
            load(b).start()
        plan(
            devices, dest_ref.shape[0] // devices, count, full, limit,
            dest_ref, shift_ref, sizes_ref, table_ref, final_ref, index_ref, offset_ref, *scratch,
        )
        own.wait()

    at = p * count + s
    load(at).wait()
    half_step(sizes_ref, basis, blocks[at], s, out_ref)


def prepare(operators, basis, dest, shift, sizes, devices, limit):
    per, sectors, width, columns = operators.shape
    pairs = devices * per
    smem = pl.BlockSpec(memory_space=pltpu.SMEM)
    return pl.pallas_call(
        functools.partial(prepare_kernel, devices, width // GRAIN, limit),
        grid=(per, sectors),
        out_shape=(
            jax.ShapeDtypeStruct((3 * limit // TILES,), jnp.int32),
            jax.ShapeDtypeStruct((3 * per,), jnp.int32),
            jax.ShapeDtypeStruct((1,), jnp.int32),
            jax.ShapeDtypeStruct((pairs,), jnp.int32),
            jax.ShapeDtypeStruct((per, sectors * width, columns), operators.dtype),
        ),
        in_specs=[smem] * 3
        + [
            pl.BlockSpec(memory_space=pl.ANY),
            pl.BlockSpec(memory_space=pl.ANY),
        ],
        out_specs=(smem,) * 4
        + (pl.BlockSpec((1, sectors * width, columns), lambda p, s: (p, 0, 0)),),
        scratch_shapes=[pltpu.SMEM((2 * pairs,), jnp.int32)] * 3
        + [pltpu.SMEM((2 * pairs + 1,), jnp.int32), pltpu.SMEM((devices * 3,), jnp.int32)]
        + [
            pltpu.VMEM(basis.shape, basis.dtype),
            pltpu.VMEM((per * sectors, width, columns), operators.dtype),
            pltpu.SemaphoreType.DMA,
            pltpu.SemaphoreType.DMA((per * sectors,)),
        ],
    )(dest, shift, sizes, basis, operators.reshape(per * sectors, width, columns))


def route_kernel(
    rounds, devices, limit, table_ref, final_ref, blocks_ref, basis_ref, out_ref, edge_ref,
    pool, stage, recv, done, own_sem, send_sem, recv_sem, edge_send, edge_recv, done_sem,
):
    own = blocks_ref.shape[0]
    per = final_ref.shape[0] // 3
    held = own // per
    me = lax.axis_index("ops")
    z, x = me // 2, me % 2
    has = (z < devices // 2 - 1, z > 0, x >= 0)
    back = (has[LEFT], has[RIGHT], has[CROSS])
    to = (me + 2, me - 2, me + 1 - 2 * x)
    count = lax.axis_size("sec")
    sec = lax.axis_index("sec")
    beside = (lax.rem(sec + 1, count), lax.rem(sec + count - 1, count))
    peers = 3 + has[RIGHT].astype(jnp.int32) + has[LEFT].astype(jnp.int32)

    load = pltpu.make_async_copy(blocks_ref, pool.at[pl.ds(0, own)], own_sem)
    load.start()
    barrier = pltpu.get_barrier_semaphore()
    for d in range(3):

        @pl.when(has[d])
        def _():
            pl.semaphore_signal(barrier, inc=1, device_id={"ops": to[d]}, device_id_type=MESH)

    for b in beside:
        pl.semaphore_signal(barrier, inc=1, device_id={"sec": b}, device_id_type=MESH)
    pl.semaphore_wait(barrier, peers)
    edges = [
        pltpu.make_async_remote_copy(
            src_ref=basis_ref.at[basis_ref.shape[0] - 1 if side == 0 else 0],
            dst_ref=edge_ref.at[side],
            send_sem=edge_send.at[side],
            recv_sem=edge_recv.at[side],
            device_id={"sec": beside[side]},
            device_id_type=MESH,
        )
        for side in range(2)
    ]
    for edge in edges:
        edge.start()
    load.wait()

    def copy(r, d):
        here, there = lax.rem(r, STAGES), lax.rem(r, SLOTS)
        return pltpu.make_async_remote_copy(
            src_ref=stage.at[here, d],
            dst_ref=recv.at[there, d],
            send_sem=send_sem.at[here, d],
            recv_sem=recv_sem.at[there, d],
            device_id={"ops": to[d]},
            device_id_type=MESH,
        )

    def sent(r):
        for d in range(3):

            @pl.when(has[d])
            def _():
                copy(r, d).wait_send()

    def send(r):
        here = lax.rem(r, STAGES)
        for d in range(3):
            word = table_ref[r * 3 + d]
            one = (word & ((1 << BITS) - 1)) - BIAS
            two = (lax.shift_right_logical(word, BITS) & ((1 << BITS) - 1)) - BIAS
            turn = lax.shift_right_logical(word, 2 * BITS)
            for t in range(TILES):
                stage[here, d, t] = pool[jnp.maximum(jnp.where(t < turn, one, two) + t, 0)]
        for d in range(3):

            @pl.when(has[d])
            def _():
                copy(r, d).start()

    def collect(r):
        there = lax.rem(r, SLOTS)
        for d in range(3):

            @pl.when(back[d])
            def _():
                copy(r, d).wait_recv()
                for t in range(TILES):
                    pool[own + d * limit + r * TILES + t] = recv[there, d, t]

    for r in range(LAG - 1):
        send(jnp.int32(r))

    def step(r, _):
        @pl.when(r >= STAGES)
        def _():
            sent(r - STAGES)

        send(r)
        collect(r - (LAG - 1))
        return 0

    lax.fori_loop(LAG - 1, rounds, step, 0)
    for r in range(rounds - LAG + 1, rounds):
        collect(jnp.int32(r))

    def store(q):
        part = pl.ds(q * held, held)
        return pltpu.make_async_copy(done.at[part], out_ref.at[part], done_sem.at[q])

    for q in range(per):
        one, two, turn = final_ref[q * 3], final_ref[q * 3 + 1], final_ref[q * 3 + 2]

        def finish(i, _):
            for u in range(4):
                k = i * 4 + u
                at = jnp.where(k < turn, one, two) + k
                done[q * held + k] = pool[jnp.clip(at, 0, own + 3 * limit)]
            return 0

        lax.fori_loop(0, held // 4, finish, 0)
        store(q).start()
    for r in range(rounds - STAGES, rounds):
        sent(jnp.int32(r))
    for edge in edges:
        edge.wait()
    for q in range(per):
        store(q).wait()


def route(rounds, devices, limit, table, final, lists, basis):
    own, _, columns = lists.shape
    dtype = lists.dtype
    smem = pl.BlockSpec(memory_space=pltpu.SMEM)
    hbm = pl.BlockSpec(memory_space=pl.ANY)
    return pl.pallas_call(
        functools.partial(route_kernel, rounds, devices, limit),
        out_shape=(
            jax.ShapeDtypeStruct(lists.shape, dtype),
            jax.ShapeDtypeStruct((2, *basis.shape[1:]), dtype),
        ),
        in_specs=[smem, smem, hbm, hbm],
        out_specs=(hbm, hbm),
        scratch_shapes=[
            pltpu.VMEM((own + 3 * limit + 1, GRAIN, columns), dtype),
            pltpu.VMEM((STAGES, 3, TILES, GRAIN, columns), dtype),
            pltpu.VMEM((SLOTS, 3, TILES, GRAIN, columns), dtype),
            pltpu.VMEM(lists.shape, dtype),
            pltpu.SemaphoreType.DMA,
            pltpu.SemaphoreType.DMA((STAGES, 3)),
            pltpu.SemaphoreType.DMA((SLOTS, 3)),
            pltpu.SemaphoreType.DMA((2,)),
            pltpu.SemaphoreType.DMA((2,)),
            pltpu.SemaphoreType.DMA((final.shape[0] // 3,)),
        ],
        compiler_params=pltpu.CompilerParams(
            collective_id=rounds, has_side_effects=True, vmem_limit_bytes=60 * 1024 * 1024
        ),
    )(table, final, lists, basis)


def edges_of(basis):
    count = lax.axis_size("sec")
    forward = [(i, (i + 1) % count) for i in range(count)]
    backward = [(target, source) for source, target in forward]
    low = lax.ppermute(basis[-1:], "sec", forward)
    high = lax.ppermute(basis[:1], "sec", backward)
    return jnp.concatenate([low, high])


def exchange(lists, dest, per):
    ops_count = lax.axis_size("ops")
    source = jnp.argsort(dest, stable=True)
    blocks = lists.reshape(per, ops_count, -1, lists.shape[2])
    spread = lax.all_to_all(blocks, "ops", split_axis=1, concat_axis=0, tiled=True)
    ordered = jnp.take(spread, source, axis=0)
    returned = lax.all_to_all(ordered, "ops", split_axis=0, concat_axis=1, tiled=True)
    return returned.reshape(lists.shape)


def reassign(operators, basis, dest, shift, sizes):
    devices = lax.axis_size("ops")
    per, sectors, width, columns = operators.shape
    own = per * sectors * (width // GRAIN)

    def plain(lists, basis):
        return exchange(lists, dest, per), edges_of(basis)

    if devices > 12 or devices % 2 or sectors != 2:
        lists = halve(operators, basis, sizes).reshape(own, GRAIN, columns)
        offsets = jnp.take(shift, jnp.argsort(dest, stable=True))
        return *plain(lists, basis), offsets
    limit = max(ROUNDS) * TILES
    table, final, index, offsets, lists = prepare(
        operators, basis, dest, shift, sizes, devices, limit
    )
    lists = lists.reshape(own, GRAIN, columns)
    branches = [functools.partial(route, r, devices, limit) for r in ROUNDS]
    branches.append(lambda table, final, lists, basis: plain(lists, basis))
    out, edge = lax.switch(index[0], branches, table, final, lists, basis)
    return out, edge, offsets


def half_step(sizes_ref, basis_ref, block, s, out_ref):
    sectors, width = basis_ref.shape[:2]
    half = lax.dot_general(
        basis_ref[s], block, (((0,), (1,)), ((), ())), preferred_element_type=jnp.float32
    )
    at = start_of(sizes_ref, sectors, s, width)
    out_ref[0, pl.ds(at, width), :] = half.astype(out_ref.dtype)


def half_kernel(sizes_ref, basis_ref, block_ref, out_ref):
    half_step(sizes_ref, basis_ref, block_ref[0, 0], pl.program_id(1), out_ref)


def start_of(sizes_ref, sectors, s, width):
    at = jnp.int32(0)
    for before in range(sectors - 1):
        size = sizes_ref[lax.axis_index("sec") * sectors + before]
        rows = lax.div(size + (GRAIN - 1), GRAIN) * GRAIN
        at = at + jnp.where(before < s, rows, 0)
    return pl.multiple_of(at, GRAIN)


def halve(operators, basis, sizes):
    per, sectors, width, columns = operators.shape
    smem = pl.BlockSpec(memory_space=pltpu.SMEM)
    return pl.pallas_call(
        half_kernel,
        grid=(per, sectors),
        out_shape=jax.ShapeDtypeStruct((per, sectors * width, columns), operators.dtype),
        in_specs=[
            smem,
            pl.BlockSpec(basis.shape, lambda p, s: (0, 0, 0)),
            pl.BlockSpec((1, 1, width, columns), lambda p, s: (p, s, 0, 0)),
        ],
        out_specs=pl.BlockSpec((1, sectors * width, columns), lambda p, s: (p, 0, 0)),
        cost_estimate=pl.CostEstimate(
            flops=2 * per * sectors * width**3, bytes_accessed=6 * operators.size,
            transcendentals=0,
        ),
    )(sizes, basis, operators)


def rotate_kernel(
    total, offset_ref, sizes_ref, edge_ref, basis_ref, list_ref, out_ref, near, sem
):
    per, sectors = pl.num_programs(0), pl.num_programs(1)
    p, s = pl.program_id(0), pl.program_id(1)
    count, width = basis_ref.shape[:2]

    @pl.when((p == 0) & (s == 0))
    def _():
        copies = [
            pltpu.make_async_copy(edge_ref.at[0], near.at[0], sem.at[0]),
            pltpu.make_async_copy(basis_ref, near.at[pl.ds(1, count)], sem.at[1]),
            pltpu.make_async_copy(edge_ref.at[1], near.at[count + 1], sem.at[2]),
        ]
        for copy in copies:
            copy.start()
        for copy in copies:
            copy.wait()

    offset = offset_ref[lax.axis_index("ops") * per + p]
    sector = lax.axis_index("sec") * sectors + s
    kept_columns = sizes_ref[sector]
    kept_rows = sizes_ref[lax.rem(sector + offset + total, total)]
    at = start_of(sizes_ref, count, s, width)
    full = lax.dot_general(
        near[1 + s + offset], list_ref[0, pl.ds(at, width), :], (((0,), (1,)), ((), ())),
        preferred_element_type=jnp.float32,
    )
    row = lax.broadcasted_iota(jnp.int32, full.shape, 0)
    column = lax.broadcasted_iota(jnp.int32, full.shape, 1)
    full = jnp.where((row < kept_rows) & (column < kept_columns), full, 0.0)
    out_ref[0, 0] = full.astype(out_ref.dtype)


def rotate(lists, basis, edge, offsets, sizes, shape, total):
    per, sectors, width, columns = shape
    smem = pl.BlockSpec(memory_space=pltpu.SMEM)
    hbm = pl.BlockSpec(memory_space=pl.ANY)
    return pl.pallas_call(
        functools.partial(rotate_kernel, total),
        grid=(per, sectors),
        out_shape=jax.ShapeDtypeStruct(shape, lists.dtype),
        in_specs=[
            smem, smem, hbm, hbm,
            pl.BlockSpec((1, sectors * width, columns), lambda p, s: (p, 0, 0)),
        ],
        out_specs=pl.BlockSpec((1, 1, width, columns), lambda p, s: (p, s, 0, 0)),
        scratch_shapes=[
            pltpu.VMEM((sectors + 2, width, columns), lists.dtype),
            pltpu.SemaphoreType.DMA((3,)),
        ],
        cost_estimate=pl.CostEstimate(
            flops=2 * per * sectors * width**3, bytes_accessed=5 * lists.size, transcendentals=0
        ),
    )(offsets, sizes, edge, basis, lists)


def body(operators, basis, shift, dest, sizes):
    per, sectors, width, columns = operators.shape
    total = sectors * lax.axis_size("sec")
    lists, edge, offsets = reassign(operators, basis, dest, shift, sizes)
    lists = lists.reshape(per, sectors * width, columns)
    return rotate(lists, basis, edge, offsets, sizes, operators.shape, total)


def solution(mesh):
    return jax.shard_map(
        body,
        mesh=mesh,
        in_specs=(P("ops", "sec", None, None), P("sec", None, None), P(), P(), P()),
        out_specs=P("ops", "sec", None, None),
        check_vma=False,
    )
```
